32 devices in a mesh: groups: 2 (over y), sample: 4 (over x, core), head: 4 (over z).
Axes of the slice: x: 2, y: 2, z: 4, core: 2. Of those that a mesh axis runs over, the one named last changes fastest.
Arguments:
- hidden_states: bfloat16 [2048, 8192], P(('groups', 'sample'), 'head'), parts along dimension 0, may hold values from -6 to 6
- response_lengths: int32 [8], P(('groups', 'sample')), parts along dimension 0, may hold values from 64 to 256
- prompt_keys: bfloat16 [16384, 512], P(('groups', 'sample'), 'head'), parts along dimension 0, may hold values from -304 to 304
- prompt_values: bfloat16 [16384, 512], P(('groups', 'sample'), 'head'), parts along dimension 0, may hold values from -24 to 24
- w_query: bfloat16 [8192, 2048], P('sample', 'head'), may hold values from -0.0625 to 0.0625
- w_key: bfloat16 [8192, 512], P('sample', 'head'), may hold values from -0.1875 to 0.1875
- w_value: bfloat16 [8192, 512], P('sample', 'head'), may hold values from -0.25 to 0.25
- w_out: bfloat16 [2048, 8192], P('head', 'sample'), may hold values from -0.375 to 0.375
Outputs:
- mixed: bfloat16 [2048, 8192], P(('groups', 'sample'), 'head'), parts along dimension 0
The draws below stay inside these ranges and needn't reach their ends.
There are 2 independent parts, one for each index of `groups`. The reference program is written for one: setup_inputs(seed, part) draws one part's arguments, and reference() takes and returns one part's arrays. A program takes and returns all parts, laid end to end along the dimension named above; an argument that names none is the same for every part. Nothing has to cross between parts.
All inputs are finite; a program needn't handle non-finite values.
Results may differ from the reference program's by a relative error of at most 0.0144.
The reference program's roundings to bfloat16 on the way count: a program that leaves them out, or rounds other values in their place, can miss the bound.
Values may be sent and summed in bfloat16 or wider, within the bound.
A program may use at most 192 MiB of HBM per device.

```python
import jax
import jax.numpy as jnp
from jax import lax

D = 8192
HD = 128
QPK = 4
RESP_TOK = 256
PROMPT = 8192
KV_HEADS = 4
RESPONSES = 4
TOKENS = 1024


def draw_prompt_keys(key, part):
    shape_all = (PROMPT, KV_HEADS * HD)
    key_base = jax.random.fold_in(key, 11)
    return jnp.clip(2.0 * jax.random.normal(key_base, shape_all, jnp.float32), -12.0, 12.0).astype(jnp.bfloat16)


def with_ends(values, stream_key, least, largest):
    index_at = [jax.random.randint(jax.random.fold_in(stream_key, axis), (), 0, length) for axis, length in enumerate(values.shape)]
    main_axis = values.shape.index(max(values.shape))
    beside = index_at[:main_axis] + [(index_at[main_axis] + 1) % values.shape[main_axis]] + index_at[main_axis + 1:]
    return values.at[tuple(index_at)].set(least).at[tuple(beside)].set(largest)


def steps_of(key, shape, cuts, smallest, high):
    level = 1.0
    for dim, blocks in cuts:
        steps = jax.random.uniform(jax.random.fold_in(jax.random.fold_in(key, 6), dim), (blocks,), jnp.float32, smallest / len(cuts), high / len(cuts))
        level = level * jnp.repeat(jnp.exp(steps), shape[dim] // blocks).reshape((-1,) + (1,) * (len(shape) - 1 - dim))
    return level


def normal_values(rng, extent, spread, most, split=(), kind=jnp.bfloat16):
    loudness = steps_of(rng, extent, split, -0.22, 0.18) if split else 1.0
    drawn = jax.random.normal(rng, extent, jnp.float32) * spread * loudness
    return jnp.minimum(jnp.maximum(drawn, -most), most).astype(kind)


def setup_inputs(seed: int = 0, part: int = 0) -> dict:
    key_of = jax.random.split(jax.random.key(seed), 9)
    part_splits = jax.random.split(jax.random.fold_in(key_of[8], part), 9)
    hidden_states = normal_values(part_splits[0], (TOKENS, D), 1.0, 6.0, ((0, 4), (1, 4)))
    response_lengths = with_ends(jax.random.randint(part_splits[1], (RESPONSES,), RESP_TOK // 4, RESP_TOK + 1), jax.random.fold_in(part_splits[1], 1), RESP_TOK // 4, RESP_TOK).astype(jnp.int32)
    prompt_keys = draw_prompt_keys(jax.random.fold_in(jax.random.fold_in(key_of[8], part), 71), part)
    prompt_values = normal_values(part_splits[3], (PROMPT, KV_HEADS * HD), 4.0, 24.0, ((0, 4), (1, 4)))
    w_query = normal_values(key_of[4], (D, KV_HEADS * QPK * HD), D ** -0.5, 0.0625, ((0, 4), (1, 4)))
    w_key = normal_values(key_of[5], (D, KV_HEADS * HD), (D // 9) ** -0.5, 0.1875, ((0, 4), (1, 4)))
    w_value = normal_values(key_of[6], (D, KV_HEADS * HD), (D // 16) ** -0.5, 0.25, ((0, 4), (1, 4)))
    w_out = normal_values(key_of[7], (KV_HEADS * QPK * HD, D), (KV_HEADS * QPK * HD // 9) ** -0.5, 0.375, ((0, 4), (1, 4)))
    return dict(hidden_states=hidden_states, response_lengths=response_lengths, prompt_keys=prompt_keys, prompt_values=prompt_values, w_query=w_query, w_key=w_key, w_value=w_value, w_out=w_out)


EPSILON = 1e-06
THETA_BASE = 1000000.0
FLOOR_SCORE = -1e+30

def rotate(values, positions):
    width_all = values.shape[-1]
    half_width = width_all // 2
    frequency = THETA_BASE ** (-(jnp.arange(half_width, dtype=jnp.float32) * 2.0) / width_all)
    angles = positions.astype(jnp.float32)[:, None] * frequency[None, :]
    cosine = jnp.cos(angles)[:, None, :]
    sine_part = jnp.sin(angles)[:, None, :]
    first_half = values[..., :half_width]
    second = values[..., half_width:]
    return jnp.concatenate([first_half * cosine - second * sine_part, second * cosine + first_half * sine_part], axis=-1)

def reference(hidden_states, response_lengths, prompt_keys, prompt_values, w_query, w_key, w_value, w_out):
    widened = hidden_states.astype(jnp.float32)
    normed = (widened * lax.rsqrt(lax.optimization_barrier(jnp.mean(widened * widened, axis=1, keepdims=True)) + EPSILON)).astype(jnp.bfloat16)
    query_raw = jnp.dot(normed, w_query, preferred_element_type=jnp.float32)
    key_raw = jnp.dot(normed, w_key, preferred_element_type=jnp.float32)
    value_raw = jnp.dot(normed, w_value, preferred_element_type=jnp.float32)
    positions = PROMPT + jnp.arange(TOKENS, dtype=jnp.int32) % RESP_TOK
    queries = rotate(query_raw.reshape(TOKENS, KV_HEADS * QPK, HD), positions).astype(jnp.bfloat16)
    keys_new = rotate(key_raw.reshape(TOKENS, KV_HEADS, HD), positions).astype(jnp.bfloat16)
    values_new = value_raw.astype(jnp.bfloat16).reshape(TOKENS, KV_HEADS, HD)
    places = jnp.arange(RESP_TOK, dtype=jnp.int32)

    def attend_pair(pair):
        response = pair // KV_HEADS
        kv_head = pair % KV_HEADS
        first_row = (response * RESP_TOK).astype(jnp.int32)
        zero_index = jnp.int32(0)
        query_block = lax.dynamic_slice(queries, (first_row, (kv_head * QPK).astype(jnp.int32), zero_index), (RESP_TOK, QPK, HD))
        key_block = lax.dynamic_slice(keys_new, (first_row, kv_head.astype(jnp.int32), zero_index), (RESP_TOK, 1, HD))[:, 0]
        value_block = lax.dynamic_slice(values_new, (first_row, kv_head.astype(jnp.int32), zero_index), (RESP_TOK, 1, HD))[:, 0]
        cached_keys = lax.dynamic_slice(prompt_keys, (zero_index, (kv_head * HD).astype(jnp.int32)), (PROMPT, HD))
        cached_values = lax.dynamic_slice(prompt_values, (zero_index, (kv_head * HD).astype(jnp.int32)), (PROMPT, HD))
        all_keys = jnp.concatenate([cached_keys, key_block], axis=0).astype(jnp.float32)
        all_values = jnp.concatenate([cached_values, value_block], axis=0).astype(jnp.float32)
        scores = jnp.einsum('tgd,kd->gtk', query_block.astype(jnp.float32), all_keys) * HD ** (-0.5)
        length = response_lengths[response]
        allowed_new = (places[None, :] <= places[:, None]) & (places[None, :] < length)
        allowed = jnp.concatenate([jnp.ones((RESP_TOK, PROMPT), dtype=bool), allowed_new], axis=1)
        scores = jnp.where(allowed[None], scores, FLOOR_SCORE)
        peak = lax.optimization_barrier(jnp.max(scores, axis=2, keepdims=True))
        exponent = jnp.exp(scores - peak)
        total = lax.optimization_barrier(jnp.sum(exponent, axis=2, keepdims=True))
        rounded = lax.optimization_barrier(exponent.astype(jnp.bfloat16))
        blended = jnp.einsum('gtk,kd->gtd', rounded.astype(jnp.float32), all_values) / total
        blended = jnp.where((places < length)[None, :, None], blended, 0.0)
        return jnp.transpose(blended, (1, 0, 2)).reshape(RESP_TOK, QPK * HD).astype(jnp.bfloat16)
    blocks = lax.map(attend_pair, jnp.arange(RESPONSES * KV_HEADS, dtype=jnp.int32))
    attended = blocks.reshape(RESPONSES, KV_HEADS, RESP_TOK, QPK * HD).transpose(0, 2, 1, 3).reshape(TOKENS, KV_HEADS * QPK * HD)
    return jnp.dot(attended, w_out, preferred_element_type=jnp.float32).astype(jnp.bfloat16)
```

```python
import functools

import jax
import jax.numpy as jnp
import numpy as np
from jax import lax
from jax.experimental import pallas as pl
from jax.experimental.pallas import tpu as pltpu
from jax.sharding import PartitionSpec as P

EPSILON = 1e-06
THETA_BASE = 1000000.0
FLOOR_SCORE = -1e30
LOG2E = 1.4426950408889634
MESH = pl.DeviceIdType.MESH
F32 = jnp.float32
BF16 = jnp.bfloat16
CORES = 2


def tables(first, count, width):
    half = width // 2
    power = -(np.arange(half, dtype=np.float32) * np.float32(2.0)) / np.float32(width)
    frequency = np.power(np.float32(THETA_BASE), power, dtype=np.float32)
    places = (first + np.arange(count)).astype(np.float32)
    angles = (places[:, None] * frequency[None, :]).astype(np.float64)
    cosine = np.cos(angles).astype(np.float32)
    sine = np.sin(angles).astype(np.float32)
    return (
        np.concatenate([cosine, cosine], axis=1),
        np.concatenate([-sine, sine], axis=1),
    )


class Copies:
    def __init__(self, send, recv):
        self.send, self.recv = send, recv
        self.bases, self.size = {}, 0

    def base(self, key, count=1):
        if key not in self.bases:
            self.bases[key] = self.size
            self.size += count
        return self.bases[key]

    def put(self, src, dst, device, sent, landed):
        return pltpu.make_async_remote_copy(
            src_ref=src,
            dst_ref=dst,
            send_sem=self.send.at[sent],
            recv_sem=self.recv.at[landed],
            device_id=device,
            device_id_type=MESH,
        )

    def make(self, key, src, dst, device):
        number = self.base(key)
        return self.put(src, dst, device, number, number)


def kernel(
    cfg,
    length_ref, cos_ref, sin_ref, hid, pk, pv, wq, wk, wv, wo,
    out,
    hbuf, wall, kvbuf, wobuf, relay, acc, qs, knew, vnew, mrow, lrow, oacc, abuf, total_out,
    send_sems, recv_sems, load_sems,
):
    G, S, N, T, D, HD, QPK = cfg["G"], cfg["S"], cfg["N"], cfg["T"], cfg["D"], cfg["HD"], cfg["QPK"]
    QW = QPK * HD
    W, DS, L = D // N, D // S, cfg["L"]
    LS = L // S
    X = S // CORES
    B = S // N
    PR = QW // (G * X)
    g = lax.axis_index("groups")
    s = lax.axis_index("sample")
    z = lax.axis_index("head")
    x, c = s // CORES, s % CORES
    copies = Copies(send_sems, recv_sems)
    sent = []
    later = []

    def dev(group=None, sample=None, head=None):
        return (
            g if group is None else group,
            s if sample is None else sample,
            z if head is None else head,
        )

    partner = x * CORES + (CORES - 1 - c)

    def xpeer(step):
        return lax.rem(x + step + X, X) * CORES + c

    loads = [
        (hid, hbuf.at[z]),
        (wq, wall.at[s, :, pl.ds(0, QW)]),
        (wk, wall.at[s, :, pl.ds(QW, HD)]),
        (wv, wall.at[s, :, pl.ds(QW + HD, HD)]),
        (pk, kvbuf.at[0, pl.ds(pl.multiple_of(s * LS, LS), LS)]),
        (pv, kvbuf.at[1, pl.ds(pl.multiple_of(s * LS, LS), LS)]),
    ]
    loads = [
        pltpu.make_async_copy(a, b, load_sems.at[i]) for i, (a, b) in enumerate(loads)
    ]
    for load in loads:
        load.start()

    barrier = pltpu.get_barrier_semaphore()
    for dz in range(N):
        for ds in range(S):
            if dz or ds:
                there = dev(sample=lax.rem(s + ds, S), head=lax.rem(z + dz, N))
                pl.semaphore_signal(barrier, inc=1, device_id=there, device_id_type=MESH)
    for dg in range(1, G):
        there = dev(group=lax.rem(g + dg, G))
        pl.semaphore_signal(barrier, inc=1, device_id=there, device_id_type=MESH)
    pl.semaphore_wait(barrier, N * S - 1 + G - 1)

    def hidden_up(t):
        block = jnp.maximum(z - t, 0)
        view = hbuf.at[block]
        return copies.make(("hu", t), view, view, dev(head=jnp.minimum(z + 1, N - 1)))

    def hidden_down(t):
        block = jnp.minimum(z + t, N - 1)
        view = hbuf.at[block]
        return copies.make(("hd", t), view, view, dev(head=jnp.maximum(z - 1, 0)))

    def hidden_send(t):
        @pl.when((z - t >= 0) & (z + 1 < N))
        def _():
            hidden_up(t).start()

        @pl.when((z + t < N) & (z > 0))
        def _():
            hidden_down(t).start()

    def arrived(key, view):
        copies.make(key, view, view, dev(sample=partner)).wait_recv()

    def hidden_pump(t):
        @pl.when(z - t >= 0)
        def _():
            arrived(("hu", t - 1), hbuf.at[jnp.maximum(z - t, 0)])

            if t < N - 1:
                @pl.when(z + 1 < N)
                def _():
                    hidden_up(t).start()

        @pl.when(z + t < N)
        def _():
            arrived(("hd", t - 1), hbuf.at[jnp.minimum(z + t, N - 1)])

            if t < N - 1:
                @pl.when(z > 0)
                def _():
                    hidden_down(t).start()

    class Flow:
        def __init__(self, name, view, rows, parts, subs):
            self.name, self.view, self.rows, self.parts, self.subs = name, view, rows, parts, subs

        def piece(self, owner, part, q):
            size = self.rows // (self.parts * self.subs)
            return self.view(owner, pl.multiple_of((part * self.subs + q) * size, size), size)

        def owner(self, dx, core=None):
            return lax.rem(x - dx + X, X) * CORES + (c if core is None else core)

        def part(self, dg):
            return lax.rem(g - dg + G, G) if self.parts > 1 else 0

        def start(self):
            for q in range(self.subs):
                for dx in range(1, X):
                    piece = self.piece(s, self.part(0), q)
                    copy = copies.make((self.name, "x", dx, q), piece, piece, dev(sample=xpeer(dx)))
                    copy.start()
                    sent.append(copy)
            whole = self.view(s, 0, self.rows)
            copy = copies.make((self.name, "own"), whole, whole, dev(sample=partner))
            copy.start()
            sent.append(copy)

        def to_core(self, dx, dg, q):
            piece = self.piece(self.owner(dx), self.part(dg), q)
            copy = copies.make((self.name, "c", dx, dg, q), piece, piece, dev(sample=partner))
            copy.start()
            sent.append(copy)

        def pump_x(self, q):
            for dx in range(1, X):
                piece = self.piece(self.owner(dx), self.part(0), q)
                arrived((self.name, "x", dx, q), piece)
                for dg in range(1, self.parts):
                    copy = copies.make(
                        (self.name, "g", dx, dg, q), piece, piece, dev(group=lax.rem(g + dg, G))
                    )
                    copy.start()
                    sent.append(copy)
                self.to_core(dx, 0, q)

        def pump_g(self, q):
            for dx in range(1, X):
                for dg in range(1, self.parts):
                    arrived((self.name, "g", dx, dg, q), self.piece(self.owner(dx), self.part(dg), q))
                    self.to_core(dx, dg, q)

        def finish(self):
            arrived((self.name, "own"), self.view(partner, 0, self.rows))
            for q in range(self.subs):
                for dx in range(1, X):
                    for dg in range(self.parts):
                        piece = self.piece(self.owner(dx, CORES - 1 - c), self.part(dg), q)
                        arrived((self.name, "c", dx, dg, q), piece)

    Q, QK = cfg["Q"], cfg["QK"]
    weights = Flow("w", lambda o, a, b: wall.at[o, pl.ds(a, b)], DS, G, Q)
    cached = Flow(
        "kv", lambda o, a, b: kvbuf.at[:, pl.ds(pl.multiple_of(o * LS + a, b), b)], LS, 1, QK
    )

    def piece_rows(gi, xi):
        return pl.ds(pl.multiple_of((gi * X + xi) * PR, PR), PR)

    def piece(h, b, gi, xi):
        return wobuf.at[h, b, piece_rows(gi, xi)]

    def mine(b):
        return lax.rem(z * B + b, CORES) == c

    def wo_number(kind, h):
        return copies.base(kind, N) + h

    def wo_copy(kind, h, b, gi, xi, device):
        view = piece(h, b, gi, xi)
        number = wo_number(kind, h)
        return copies.put(view, view, device, number, number)

    def begin(cond, make):
        later.append((cond, make))

        @pl.when(cond)
        def _():
            make().start()

    def gsrc(dg):
        return lax.rem(g - dg + G, G)

    def xsrc(dx):
        return lax.rem(x - dx + X, X)

    def to_x(h, b, dx, dg):
        return functools.partial(
            wo_copy, ("wx", b, dx, dg), h, b, gsrc(dg), x, dev(sample=xpeer(dx))
        )

    def to_g(h, b, dx, dg):
        return functools.partial(
            wo_copy, ("wg", b, dx, dg), h, b, g, xsrc(dx), dev(group=lax.rem(g + dg, G))
        )

    def to_c(h, b, dx, dg):
        return functools.partial(
            wo_copy, ("wc", b, dx, dg), h, b, gsrc(dg), xsrc(dx), dev(sample=partner)
        )

    def landed(kind, h, b, gi, xi):
        view = piece(h, b, gi, xi)
        number = wo_number(kind, h)
        copies.put(view, view, dev(sample=partner), number, number).wait_recv()

    def sources(t):
        if t == 0:
            return [(z, z >= 0)]
        return [(jnp.maximum(z - t, 0), z - t >= 0), (jnp.minimum(z + t, N - 1), z + t < N)]

    home = s // B == z
    own_wo = pltpu.make_async_copy(
        wo.at[piece_rows(g, x)], piece(z, lax.rem(s, B), g, x), load_sems.at[len(loads)]
    )

    def stage_z(t):
        for h, valid in sources(t):
            for b in range(B):
                cond = valid & mine(b)

                @pl.when(cond)
                def _():
                    if t == 0:
                        source = home & (lax.rem(s, B) == b)

                        @pl.when(source)
                        def _():
                            own_wo.wait()

                        @pl.when(jnp.logical_not(source))
                        def _():
                            landed(("wz", b), h, b, g, x)
                    else:
                        landed(("wz", b), h, b, g, x)
                for dx in range(1, X):
                    begin(cond, to_x(h, b, dx, 0))
                for dg in range(1, G):
                    begin(cond, to_g(h, b, 0, dg))
                begin(cond, to_c(h, b, 0, 0))

    def stage_xg(t):
        for h, valid in sources(t):
            for b in range(B):
                cond = valid & mine(b)
                for dx in range(1, X):
                    @pl.when(cond)
                    def _():
                        landed(("wx", b, dx, 0), h, b, g, xsrc(dx))
                    if t % 2:
                        for dg in range(1, G):
                            begin(cond, to_g(h, b, dx, dg))
                    begin(cond, to_c(h, b, dx, 0))
                for dg in range(1, G):
                    @pl.when(cond)
                    def _():
                        landed(("wg", b, 0, dg), h, b, gsrc(dg), x)
                    if not t % 2:
                        for dx in range(1, X):
                            begin(cond, to_x(h, b, dx, dg))
                    begin(cond, to_c(h, b, 0, dg))

    def stage_d(t):
        for h, valid in sources(t):
            for b in range(B):
                cond = valid & mine(b)
                for dx in range(1, X):
                    for dg in range(1, G):
                        @pl.when(cond)
                        def _():
                            kind = "wg" if t % 2 else "wx"
                            landed((kind, b, dx, dg), h, b, gsrc(dg), xsrc(dx))
                        begin(cond, to_c(h, b, dx, dg))

    def stage_f(t):
        for h, valid in sources(t):
            for b in range(B):
                @pl.when(valid & jnp.logical_not(mine(b)))
                def _():
                    for dx in range(X):
                        for dg in range(G):
                            landed(("wc", b, dx, dg), h, b, gsrc(dg), xsrc(dx))

    def cross(dx):
        to = lax.rem(x + dx, X)
        number = copies.base(("wr", dx))
        return copies.put(
            wo.at[piece_rows(g, to)], relay.at[dx - 1], dev(sample=xpeer(dx)), number, number
        )

    def cross_home(dx):
        to = lax.rem(x + dx, X)
        b = lax.rem(s, B)
        return copies.put(
            wo.at[piece_rows(g, to)], piece(z, b, g, to), dev(sample=xpeer(dx)),
            copies.base(("wr", dx)), copies.base(("wz", 0), N * B) + b * N + z,
        )

    def along(dx):
        o = xsrc(dx) * CORES + c
        p, b = o // B, lax.rem(o, B)
        src = wo.at[piece_rows(g, x)] if dx == 0 else relay.at[dx - 1]
        landing = copies.base(("wz", 0), N * B) + b * N + z
        return copies.put(
            src, piece(z, b, g, x), dev(head=p), copies.base(("wzs", dx)), landing
        )

    for b in range(1, B):
        copies.bases[("wz", b)] = copies.base(("wz", 0), N * B) + b * N
    copies.base(("wz", 0), N * B)

    def inject(stage):
        end = (z == 0) | (z == N - 1)
        for dx in range(X):
            p = (xsrc(dx) * CORES + c) // B
            far = jnp.abs(p - z)
            when = jnp.where(end & (far == 1), 1, jnp.where(end & (far < N - 1), 2, 3))
            if dx:
                when = jnp.maximum(when, 2)
            cond = (far > 0) & (when == stage)
            if dx:
                @pl.when(cond)
                def _():
                    number = copies.base(("wr", dx))
                    view = relay.at[dx - 1]
                    copies.put(view, view, dev(sample=partner), number, number).wait_recv()
            begin(cond, functools.partial(along, dx))

    loads[0].wait()
    hidden_send(0)
    for i in (1, 2, 3):
        loads[i].wait()
    weights.start()
    for dx in range(1, X):
        begin(jnp.logical_not(home), functools.partial(cross, dx))
        begin(home, functools.partial(cross_home, dx))

    @pl.when(home)
    def _():
        own_wo.start()
    for i in (4, 5):
        loads[i].wait()
    cached.start()

    mrow[...] = jnp.full_like(mrow, FLOOR_SCORE)
    lrow[...] = jnp.zeros_like(lrow)
    oacc[...] = jnp.zeros_like(oacc)

    jobs = []
    for q in range(Q):
        jobs.append(((q + 1) * 8.4 * 4 / Q, functools.partial(weights.pump_x, q)))
        jobs.append(((q + 2) * 8.4 * 4 / Q + 0.5, functools.partial(weights.pump_g, q)))
    for t in range(1, N):
        jobs.append((t * 22.0, functools.partial(hidden_pump, t)))
    for q in range(QK):
        jobs.append((45 + (q + 1) * 22.0 / QK, functools.partial(cached.pump_x, q)))
    jobs.append((24, functools.partial(inject, 1)))
    jobs.append((47, functools.partial(inject, 2)))
    jobs.append((46.5, functools.partial(stage_z, 0)))
    jobs.append((58, functools.partial(stage_xg, 0)))
    jobs.append((64, functools.partial(stage_d, 0)))
    jobs.sort(key=lambda job: job[0])
    for _, job in jobs:
        job()
    weights.finish()
    inject(3)

    def squares(i, total):
        h = hbuf[i].astype(F32)
        h = h * h
        for j in range(W // 128):
            total = total + h[:, j * 128:(j + 1) * 128]
        return total

    total = lax.fori_loop(0, N, squares, jnp.zeros((T, 128), F32))
    total = jnp.sum(total, axis=1, keepdims=True)
    factor = lax.rsqrt(total * (1.0 / D) + EPSILON)

    tk = cfg["tk"]
    acc[...] = jnp.zeros_like(acc)

    def project(i, _):
        h = hbuf[i * tk // W, :, pl.ds(pl.multiple_of(i * tk % W, tk), tk)].astype(F32)
        n = (h * factor).astype(BF16)
        w = wall[i * tk // DS, pl.ds(pl.multiple_of(i * tk % DS, tk), tk), :]
        acc[...] += jnp.dot(n, w, preferred_element_type=F32)
        return 0

    lax.fori_loop(0, D // tk, project, 0)
    cosine, sine = cos_ref[...], sin_ref[...]

    def rope(v):
        return (v * cosine + pltpu.roll(v, HD // 2, 1) * sine).astype(BF16)

    for head in range(QPK):
        qs[head] = rope(acc[:, head * HD:(head + 1) * HD])
    knew[...] = rope(acc[:, QW:QW + HD])
    vnew[...] = acc[:, QW + HD:].astype(BF16)

    cached.finish()
    scale = (HD ** -0.5) * LOG2E
    contract = (((1,), (1,)), ((), ()))

    def score(head, keys):
        return lax.dot_general(qs[head], keys, contract, preferred_element_type=F32)

    def merge(head, scores, values):
        width = scores.shape[1]
        m_old = mrow[head]
        m_new = jnp.maximum(m_old, jnp.max(scores, axis=1, keepdims=True))
        fix = jnp.exp2((m_old - m_new) * scale)
        e = jnp.exp2((scores - m_new[:, :1]) * scale)
        l_new = lrow[head] * fix
        for j in range(width // HD):
            l_new = l_new + e[:, j * HD:(j + 1) * HD]
        oacc[head] = oacc[head] * fix + jnp.dot(
            e.astype(BF16), values, preferred_element_type=F32
        )
        mrow[head] = m_new
        lrow[head] = l_new

    kt = cfg["kt"]
    steps = L // kt
    pumps = []
    for t in range(1, N):
        pumps.append((2 * t, functools.partial(stage_z, t)))
        pumps.append((2 * t + 1, functools.partial(stage_xg, t)))
        pumps.append((2 * t + 2, functools.partial(stage_d, t)))
    pumps.sort(key=lambda pump: pump[0])

    def attend(i):
        rows = pl.ds(pl.multiple_of(i * kt, kt), kt)
        keys, values = kvbuf[0, rows, :], kvbuf[1, rows, :]
        ahead = score(0, keys)
        for head in range(QPK):
            scores = ahead
            if head + 1 < QPK:
                ahead = score(head + 1, keys)
            merge(head, scores, values)

    for i in range(steps):
        attend(i)
        for key, pump in pumps:
            if key == i + 2:
                pump()

    length = length_ref[0]
    token = lax.broadcasted_iota(jnp.int32, (T, T), 0)
    place = lax.broadcasted_iota(jnp.int32, (T, T), 1)
    allowed = (place <= token) & (place < length)
    live = lax.broadcasted_iota(jnp.int32, (T, HD), 0) < length
    keys, values = knew[...], vnew[...]
    for head in range(QPK):
        scores = score(head, keys)
        merge(head, jnp.where(allowed, scores, FLOOR_SCORE), values)
        whole = jnp.sum(lrow[head], axis=1, keepdims=True)
        blended = jnp.where(live, oacc[head] / whole, 0.0)
        abuf[z, :, head * HD:(head + 1) * HD] = blended.astype(BF16)

    def attended(t, sign):
        to = jnp.maximum(z - t, 0) if sign < 0 else jnp.minimum(z + t, N - 1)
        view = abuf.at[z]
        return copies.put(
            view, view, dev(head=to), copies.base(("as", t, sign)), copies.base("a", N) + z
        )

    for t in range(N - 1, 0, -1):
        begin(z + t < N, functools.partial(attended, t, 1))
        begin(z - t >= 0, functools.partial(attended, t, -1))

    tn = cfg["tn"]

    def product(t):
        for h, valid in sources(t):
            @pl.when(valid)
            def _():
                if t:
                    view = abuf.at[h]
                    number = copies.base("a", N) + h
                    copies.put(view, view, dev(sample=partner), number, number).wait_recv()

                def tile(i, _):
                    cols = pl.ds(pl.multiple_of(i * tn, tn), tn)
                    w = wobuf[h, i * tn // DS, :, pl.ds(pl.multiple_of(i * tn % DS, tn), tn)]
                    part = jnp.dot(abuf[h], w, preferred_element_type=F32)
                    total_out[:, cols] = part if t == 0 else total_out[:, cols] + part
                    return 0

                lax.fori_loop(0, W // tn, tile, 0)

    ready = 0
    for key in range(steps + 2, 2 * N + 1):
        for other, pump in pumps:
            if other == key:
                pump()
        while ready < N and 2 * ready + 2 < key:
            stage_f(ready)
            product(ready)
            ready += 1
    while ready < N:
        stage_f(ready)
        product(ready)
        ready += 1
    out[...] = total_out[...].astype(BF16)

    for copy in sent:
        copy.wait_send()
    for t in range(N - 1):
        @pl.when((z - t >= 0) & (z + 1 < N))
        def _():
            hidden_up(t).wait_send()

        @pl.when((z + t < N) & (z > 0))
        def _():
            hidden_down(t).wait_send()
    for cond, make in later:
        @pl.when(cond)
        def _():
            make().wait_send()


def per_device(cfg, *args):
    hidden, lengths, pk, pv, wq, wk, wv, wo = args
    T, W = hidden.shape
    HD = pk.shape[1]
    QW = wq.shape[1]
    G, S, N = cfg["G"], cfg["S"], cfg["N"]
    D = W * N
    X = S // CORES
    B = S // N
    L = pk.shape[0] * S
    DS = D // S
    Q = max(1, 4 // max(1, X - 1))
    QK = max(1, 2 // max(1, X - 1))
    cfg = dict(
        cfg, T=T, D=D, HD=HD, QPK=QW // HD, L=L, Q=Q, QK=QK,
        tk=min(2048, W, DS), kt=min(2048, L), tn=min(512, W, DS),
    )
    QPK = QW // HD
    cosine, sine = tables(L, T, HD)
    copies = (
        2 + (X - 1) * Q * 2 * G + (X - 1) * QK * 2 + 2 * N
        + N * B * (1 + 3 * X * G) + 2 * X + X * (1 + B) + N + 2 * N
    )
    anywhere = pl.BlockSpec(memory_space=pl.ANY)
    vmem = pl.BlockSpec(memory_space=pltpu.VMEM)
    return pl.pallas_call(
        functools.partial(kernel, cfg),
        out_shape=jax.ShapeDtypeStruct((T, W), BF16),
        in_specs=[pl.BlockSpec(memory_space=pltpu.SMEM), vmem, vmem] + [anywhere] * 7,
        out_specs=vmem,
        scratch_shapes=[
            pltpu.VMEM((N, T, W), BF16),
            pltpu.VMEM((S, DS, QW + 2 * HD), BF16),
            pltpu.VMEM((2, L, HD), BF16),
            pltpu.VMEM((N, B, QW, DS), BF16),
            pltpu.VMEM((max(1, X - 1), QW // (G * X), DS), BF16),
            pltpu.VMEM((T, QW + 2 * HD), F32),
            pltpu.VMEM((QPK, T, HD), BF16),
            pltpu.VMEM((T, HD), BF16),
            pltpu.VMEM((T, HD), BF16),
            pltpu.VMEM((QPK, T, HD), F32),
            pltpu.VMEM((QPK, T, HD), F32),
            pltpu.VMEM((QPK, T, HD), F32),
            pltpu.VMEM((N, T, QW), BF16),
            pltpu.VMEM((T, W), F32),
            pltpu.SemaphoreType.DMA((copies,)),
            pltpu.SemaphoreType.DMA((copies,)),
            pltpu.SemaphoreType.DMA((7,)),
        ],
        compiler_params=pltpu.CompilerParams(
            collective_id=0, has_side_effects=True, vmem_limit_bytes=64_000_000
        ),
    )(lengths, jnp.asarray(cosine), jnp.asarray(sine), hidden, pk, pv, wq, wk, wv, wo)


def solution(mesh):
    cfg = dict(G=mesh.shape["groups"], S=mesh.shape["sample"], N=mesh.shape["head"])
    rows = P(("groups", "sample"), "head")
    placed = (
        rows, P(("groups", "sample")), rows, rows,
        P("sample", "head"), P("sample", "head"), P("sample", "head"), P("head", "sample"),
    )
    return jax.shard_map(
        functools.partial(per_device, cfg),
        mesh=mesh,
        in_specs=placed,
        out_specs=rows,
        check_vma=False,
    )
```

```python
import functools

import jax
import jax.numpy as jnp
import numpy as np
from jax import lax
from jax.experimental import pallas as pl
from jax.experimental.pallas import tpu as pltpu
from jax.sharding import PartitionSpec as P

EPSILON = 1e-06
THETA_BASE = 1000000.0
FLOOR_SCORE = -1e30
LOG2E = 1.4426950408889634
MESH = pl.DeviceIdType.MESH
F32 = jnp.float32
BF16 = jnp.bfloat16
CORES = 2


def tables(first, count, width):
    half = width // 2
    power = -(np.arange(half, dtype=np.float32) * np.float32(2.0)) / np.float32(width)
    frequency = np.power(np.float32(THETA_BASE), power, dtype=np.float32)
    places = (first + np.arange(count)).astype(np.float32)
    angles = (places[:, None] * frequency[None, :]).astype(np.float64)
    cosine = np.cos(angles).astype(np.float32)
    sine = np.sin(angles).astype(np.float32)
    return (
        np.concatenate([cosine, cosine], axis=1),
        np.concatenate([-sine, sine], axis=1),
    )


class Copies:
    def __init__(self, send, recv):
        self.send, self.recv = send, recv
        self.bases, self.size = {}, 0

    def base(self, key, count=1):
        if key not in self.bases:
            self.bases[key] = self.size
            self.size += count
        return self.bases[key]

    def put(self, src, dst, device, sent, landed):
        return pltpu.make_async_remote_copy(
            src_ref=src,
            dst_ref=dst,
            send_sem=self.send.at[sent],
            recv_sem=self.recv.at[landed],
            device_id=device,
            device_id_type=MESH,
        )

    def make(self, key, src, dst, device):
        number = self.base(key)
        return self.put(src, dst, device, number, number)


def kernel(
    cfg,
    length_ref, cos_ref, sin_ref, hid, pk, pv, wq, wk, wv, wo,
    out,
    hbuf, wall, kvbuf, wobuf, relay, acc, qs, knew, vnew, mrow, lrow, oacc, abuf, total_out,
    stats, rows,
    send_sems, recv_sems, load_sems,
):
    G, S, N, T, D, HD, QPK = cfg["G"], cfg["S"], cfg["N"], cfg["T"], cfg["D"], cfg["HD"], cfg["QPK"]
    QW = QPK * HD
    W, DS, L = D // N, D // S, cfg["L"]
    LS = L // S
    X = S // CORES
    B = S // N
    PR = QW // (G * X)
    g = lax.axis_index("groups")
    s = lax.axis_index("sample")
    z = lax.axis_index("head")
    x, c = s // CORES, s % CORES
    copies = Copies(send_sems, recv_sems)
    sent = []
    later = []

    def dev(group=None, sample=None, head=None):
        return (
            g if group is None else group,
            s if sample is None else sample,
            z if head is None else head,
        )

    partner = x * CORES + (CORES - 1 - c)

    def xpeer(step):
        return lax.rem(x + step + X, X) * CORES + c

    loads = [
        (hid, hbuf.at[z]),
        (wq, wall.at[s, :, pl.ds(0, QW)]),
        (wk, wall.at[s, :, pl.ds(QW, HD)]),
        (wv, wall.at[s, :, pl.ds(QW + HD, HD)]),
        (pk, kvbuf.at[0, pl.ds(pl.multiple_of(s * LS, LS), LS)]),
        (pv, kvbuf.at[1, pl.ds(pl.multiple_of(s * LS, LS), LS)]),
    ]
    loads = [
        pltpu.make_async_copy(a, b, load_sems.at[i]) for i, (a, b) in enumerate(loads)
    ]
    for load in loads:
        load.start()

    barrier = pltpu.get_barrier_semaphore()
    for dz in range(N):
        for ds in range(S):
            if dz or ds:
                there = dev(sample=lax.rem(s + ds, S), head=lax.rem(z + dz, N))
                pl.semaphore_signal(barrier, inc=1, device_id=there, device_id_type=MESH)
    for dg in range(1, G):
        there = dev(group=lax.rem(g + dg, G))
        pl.semaphore_signal(barrier, inc=1, device_id=there, device_id_type=MESH)
    with jax.named_scope("barrier"):
        pl.semaphore_wait(barrier, N * S - 1 + G - 1)

    def hidden_up(t):
        block = jnp.maximum(z - t, 0)
        view = hbuf.at[block]
        return copies.make(("hu", t), view, view, dev(head=jnp.minimum(z + 1, N - 1)))

    def hidden_down(t):
        block = jnp.minimum(z + t, N - 1)
        view = hbuf.at[block]
        return copies.make(("hd", t), view, view, dev(head=jnp.maximum(z - 1, 0)))

    def hidden_send(t):
        @pl.when((z - t >= 0) & (z + 1 < N))
        def _():
            hidden_up(t).start()

        @pl.when((z + t < N) & (z > 0))
        def _():
            hidden_down(t).start()

    def arrived(key, view):
        copies.make(key, view, view, dev(sample=partner)).wait_recv()

    def hidden_pump(t):
        @pl.when(z - t >= 0)
        def _():
            arrived(("hu", t - 1), hbuf.at[jnp.maximum(z - t, 0)])

            if t < N - 1:
                @pl.when(z + 1 < N)
                def _():
                    hidden_up(t).start()

        @pl.when(z + t < N)
        def _():
            arrived(("hd", t - 1), hbuf.at[jnp.minimum(z + t, N - 1)])

            if t < N - 1:
                @pl.when(z > 0)
                def _():
                    hidden_down(t).start()

    class Flow:
        def __init__(self, name, view, rows, parts, subs):
            self.name, self.view, self.rows, self.parts, self.subs = name, view, rows, parts, subs

        def piece(self, owner, part, q):
            size = self.rows // (self.parts * self.subs)
            return self.view(owner, pl.multiple_of((part * self.subs + q) * size, size), size)

        def owner(self, dx, core=None):
            return lax.rem(x - dx + X, X) * CORES + (c if core is None else core)

        def part(self, dg):
            return lax.rem(g - dg + G, G) if self.parts > 1 else 0

        def start(self):
            for q in range(self.subs):
                for dx in range(1, X):
                    piece = self.piece(s, self.part(0), q)
                    copy = copies.make((self.name, "x", dx, q), piece, piece, dev(sample=xpeer(dx)))
                    copy.start()
                    sent.append(copy)
            whole = self.view(s, 0, self.rows)
            copy = copies.make((self.name, "own"), whole, whole, dev(sample=partner))
            copy.start()
            sent.append(copy)

        def to_core(self, dx, dg, q):
            piece = self.piece(self.owner(dx), self.part(dg), q)
            copy = copies.make((self.name, "c", dx, dg, q), piece, piece, dev(sample=partner))
            copy.start()
            sent.append(copy)

        def pump_x(self, q):
            for dx in range(1, X):
                piece = self.piece(self.owner(dx), self.part(0), q)
                arrived((self.name, "x", dx, q), piece)
                for dg in range(1, self.parts):
                    copy = copies.make(
                        (self.name, "g", dx, dg, q), piece, piece, dev(group=lax.rem(g + dg, G))
                    )
                    copy.start()
                    sent.append(copy)
                self.to_core(dx, 0, q)

        def pump_g(self, q):
            for dx in range(1, X):
                for dg in range(1, self.parts):
                    arrived((self.name, "g", dx, dg, q), self.piece(self.owner(dx), self.part(dg), q))
                    self.to_core(dx, dg, q)

        def finish_own(self):
            arrived((self.name, "own"), self.view(partner, 0, self.rows))

        def finish_rest(self):
            for q in range(self.subs):
                for dx in range(1, X):
                    for dg in range(self.parts):
                        piece = self.piece(self.owner(dx, CORES - 1 - c), self.part(dg), q)
                        arrived((self.name, "c", dx, dg, q), piece)

    Q, QK = cfg["Q"], cfg["QK"]
    weights = Flow("w", lambda o, a, b: wall.at[o, pl.ds(a, b)], DS, G, Q)
    cached = Flow(
        "kv", lambda o, a, b: kvbuf.at[:, pl.ds(pl.multiple_of(o * LS + a, b), b)], LS, 1, QK
    )

    def outer(place):
        return (place == 0) | (place == N - 1)

    def piece_rows(gi, xi):
        return pl.ds(pl.multiple_of((gi * X + xi) * PR, PR), PR)

    def piece(h, b, gi, xi):
        return wobuf.at[h, b, piece_rows(gi, xi)]

    def mine(b):
        return lax.rem(z * B + b, CORES) == c

    def wo_number(kind, h):
        return copies.base(kind, N) + h

    def wo_copy(kind, h, b, gi, xi, device):
        view = piece(h, b, gi, xi)
        number = wo_number(kind, h)
        return copies.put(view, view, device, number, number)

    def begin(cond, make):
        later.append((cond, make))

        @pl.when(cond)
        def _():
            make().start()

    def gsrc(dg):
        return lax.rem(g - dg + G, G)

    def xsrc(dx):
        return lax.rem(x - dx + X, X)

    def to_x(h, b, dx, dg):
        return functools.partial(
            wo_copy, ("wx", b, dx, dg), h, b, gsrc(dg), x, dev(sample=xpeer(dx))
        )

    def to_g(h, b, dx, dg):
        return functools.partial(
            wo_copy, ("wg", b, dx, dg), h, b, g, xsrc(dx), dev(group=lax.rem(g + dg, G))
        )

    def to_c(h, b, dx, dg):
        return functools.partial(
            wo_copy, ("wc", b, dx, dg), h, b, gsrc(dg), xsrc(dx), dev(sample=partner)
        )

    def landed(kind, h, b, gi, xi):
        view = piece(h, b, gi, xi)
        number = wo_number(kind, h)
        copies.put(view, view, dev(sample=partner), number, number).wait_recv()

    def sources(t):
        if t == 0:
            return [(z, z >= 0)]
        return [(jnp.maximum(z - t, 0), z - t >= 0), (jnp.minimum(z + t, N - 1), z + t < N)]

    HR = QW // G
    home = s // B == z
    home_block = wobuf.at[z, lax.rem(s, B)]
    own_wo = pltpu.make_async_copy(wo, home_block, load_sems.at[len(loads)])

    def home_rows(gi):
        return pl.ds(pl.multiple_of(gi * HR, HR), HR)

    def at_home(b):
        return x == (z * B + b) // CORES

    def home_x(dx):
        landing = copies.base("oh", B) + lax.rem(s, B)
        return copies.put(
            wo.at[home_rows(g)], home_block.at[home_rows(g)], dev(sample=xpeer(dx)),
            copies.base(("ohs", dx)), landing,
        )

    def home_own():
        landing = copies.base("oo", B) + lax.rem(s, B)
        return copies.put(wo, home_block, dev(sample=partner), copies.base("oos"), landing)

    def home_copy(key, b, gi, device):
        view = wobuf.at[z, b, home_rows(gi)]
        return copies.make(key, view, view, device)

    def home_landed(number, view):
        copies.put(view, view, dev(sample=partner), number, number).wait_recv()

    def stage_home_x():
        for b in range(B):
            cond = mine(b) & jnp.logical_not(at_home(b))

            @pl.when(cond)
            def _():
                home_landed(copies.base("oh", B) + b, wobuf.at[z, b, home_rows(g)])
            for dg in range(1, G):
                begin(cond, functools.partial(
                    home_copy, ("og", b, dg), b, g, dev(group=lax.rem(g + dg, G))
                ))
            begin(cond, functools.partial(home_copy, ("oc", b, 0), b, g, dev(sample=partner)))

    def stage_home_y():
        for b in range(B):
            cond = mine(b) & jnp.logical_not(at_home(b))
            for dg in range(1, G):
                @pl.when(cond)
                def _():
                    number = copies.base(("og", b, dg))
                    home_landed(number, wobuf.at[z, b, home_rows(gsrc(dg))])
                begin(cond, functools.partial(
                    home_copy, ("oc", b, dg), b, gsrc(dg), dev(sample=partner)
                ))

    def home_finish():
        @pl.when(home)
        def _():
            own_wo.wait()
        for b in range(B):
            @pl.when(jnp.logical_not(mine(b)) & at_home(b))
            def _():
                home_landed(copies.base("oo", B) + b, wobuf.at[z, b])

            @pl.when(jnp.logical_not(mine(b)) & jnp.logical_not(at_home(b)))
            def _():
                for dg in range(G):
                    number = copies.base(("oc", b, dg))
                    home_landed(number, wobuf.at[z, b, home_rows(gsrc(dg))])

    def stage_z(t, outer_plane):
        for h, valid in sources(t):
            for b in range(B):
                cond = valid & mine(b) & (outer(z) == outer_plane)

                @pl.when(cond)
                def _():
                    landed(("wz", b), h, b, g, x)
                for dx in range(1, X):
                    begin(cond, to_x(h, b, dx, 0))
                for dg in range(1, G):
                    begin(cond, to_g(h, b, 0, dg))
                begin(cond, to_c(h, b, 0, 0))

    def stage_xg(t, outer_plane):
        for h, valid in sources(t):
            for b in range(B):
                cond = valid & mine(b) & (outer(z) == outer_plane)
                for dx in range(1, X):
                    @pl.when(cond)
                    def _():
                        landed(("wx", b, dx, 0), h, b, g, xsrc(dx))
                    if t % 2:
                        for dg in range(1, G):
                            begin(cond, to_g(h, b, dx, dg))
                    begin(cond, to_c(h, b, dx, 0))
                for dg in range(1, G):
                    @pl.when(cond)
                    def _():
                        landed(("wg", b, 0, dg), h, b, gsrc(dg), x)
                    if not t % 2:
                        for dx in range(1, X):
                            begin(cond, to_x(h, b, dx, dg))
                    begin(cond, to_c(h, b, 0, dg))

    def stage_d(t, outer_plane):
        for h, valid in sources(t):
            for b in range(B):
                cond = valid & mine(b) & (outer(z) == outer_plane)
                for dx in range(1, X):
                    for dg in range(1, G):
                        @pl.when(cond)
                        def _():
                            kind = "wg" if t % 2 else "wx"
                            landed((kind, b, dx, dg), h, b, gsrc(dg), xsrc(dx))
                        begin(cond, to_c(h, b, dx, dg))

    def stage_f(t):
        for h, valid in sources(t):
            for b in range(B):
                @pl.when(valid & jnp.logical_not(mine(b)))
                def _():
                    for dx in range(X):
                        for dg in range(G):
                            landed(("wc", b, dx, dg), h, b, gsrc(dg), xsrc(dx))

    def cross(dx):
        to = lax.rem(x + dx, X)
        number = copies.base(("wr", dx))
        return copies.put(
            wo.at[piece_rows(g, to)], relay.at[dx - 1], dev(sample=xpeer(dx)), number, number
        )

    def along(dx):
        o = xsrc(dx) * CORES + c
        p, b = o // B, lax.rem(o, B)
        src = wo.at[piece_rows(g, x)] if dx == 0 else relay.at[dx - 1]
        landing = copies.base(("wz", 0), N * B) + b * N + z
        return copies.put(
            src, piece(z, b, g, x), dev(head=p), copies.base(("wzs", dx)), landing
        )

    for b in range(1, B):
        copies.bases[("wz", b)] = copies.base(("wz", 0), N * B) + b * N
    copies.base(("wz", 0), N * B)

    def inject(stage):
        end = (z == 0) | (z == N - 1)
        for dx in range(X):
            p = (xsrc(dx) * CORES + c) // B
            far = jnp.abs(p - z)
            early = jnp.where(far == 1, 1, jnp.where(far < N - 1, 2, 4))
            when = jnp.where(end, early, 2)
            if dx:
                when = jnp.maximum(when, 2)
            cond = (far > 0) & (when == stage)
            if dx:
                @pl.when(cond)
                def _():
                    number = copies.base(("wr", dx))
                    view = relay.at[dx - 1]
                    copies.put(view, view, dev(sample=partner), number, number).wait_recv()
            begin(cond, functools.partial(along, dx))

    loads[0].wait()
    hidden_send(0)
    for i in (1, 2, 3):
        loads[i].wait()
    weights.start()
    for dx in range(1, X):
        begin(home, functools.partial(home_x, dx))
    begin(home, home_own)

    @pl.when(home)
    def _():
        own_wo.start()
    for dx in range(1, X):
        begin(jnp.logical_not(home), functools.partial(cross, dx))
    for i in (4, 5):
        loads[i].wait()
    cached.start()

    mrow[...] = jnp.full_like(mrow, FLOOR_SCORE)
    lrow[...] = jnp.zeros_like(lrow)
    oacc[...] = jnp.zeros_like(oacc)

    tk = cfg["tk"]

    def stats_copy(step):
        view = stats.at[z]
        landing = copies.base("st", N) + z
        there = dev(head=lax.rem(z + step, N))
        return copies.put(view, view, there, copies.base(("sts", step)), landing)

    def stats_send():
        part = jnp.zeros((T, 128), F32)
        for j in range(W // 128):
            h = hbuf[z, :, j * 128:(j + 1) * 128].astype(F32)
            part = part + h * h
        part = jnp.sum(jnp.transpose(part), axis=0, keepdims=True)
        stats[z] = jnp.broadcast_to(part, (8, T))
        for step in range(1, N):
            stats_copy(step).start()

    def stats_factor():
        for step in range(1, N):
            h = lax.rem(z + step, N)
            view = stats.at[h]
            number = copies.base("st", N) + h
            copies.put(view, view, dev(sample=partner), number, number).wait_recv()
        total = stats[0]
        for h in range(1, N):
            total = total + stats[h]
        scale = lax.rsqrt(total * (1.0 / D) + EPSILON)
        rows[...] = jnp.transpose(jnp.broadcast_to(scale[:1], (128, T)))

    def project(t):
        for h, valid in sources(t):
            @pl.when(valid)
            def _():
                factor = rows[:, :1]

                def part(i, _):
                    first = h * W + i * tk
                    n = hbuf[h, :, pl.ds(pl.multiple_of(i * tk, tk), tk)].astype(F32)
                    n = (n * factor).astype(BF16)
                    w = wall[first // DS, pl.ds(pl.multiple_of(first % DS, tk), tk), :]
                    dot = jnp.dot(n, w, preferred_element_type=F32)
                    acc[...] = dot + (acc[...] if t else jnp.where(i > 0, acc[...], 0.0))
                    return 0

                lax.fori_loop(0, W // tk, part, 0)

    def project_early():
        weights.finish_own()
        weights.finish_rest()
        stats_factor()
        for t in range(N - 1):
            project(t)

    jobs = []
    for q in range(Q):
        jobs.append(((q + 1) * 8.4 * 4 / Q, functools.partial(weights.pump_x, q)))
        jobs.append(((q + 2) * 8.4 * 4 / Q + 0.5, functools.partial(weights.pump_g, q)))
    for t in range(1, N):
        jobs.append((t * 22.0, functools.partial(hidden_pump, t)))
    for q in range(QK - 1):
        jobs.append((51 + (q + 1) * 22.0 / QK, functools.partial(cached.pump_x, q)))
    jobs.append((24, functools.partial(inject, 1)))
    jobs.append((47, stage_home_x))
    jobs.append((52, functools.partial(inject, 2)))
    for t in range(2, N - 1):
        jobs.append((65 - t / N, functools.partial(stage_z, t, True)))
    for t in range(1, N - 1):
        jobs.append((63 + t / N, functools.partial(stage_z, t, False)))
    jobs.append((1, stats_send))
    jobs.append((max(60, (N - 2) * 22 + 1), project_early))
    jobs.append((65.2, functools.partial(cached.pump_x, QK - 1)))
    jobs.sort(key=lambda job: job[0])
    for when, job in jobs:
        with jax.named_scope(f"job_{when}"):
            job()
    with jax.named_scope("project"):
        project(N - 1)
    cosine, sine = cos_ref[...], sin_ref[...]

    def rope(v):
        return (v * cosine + pltpu.roll(v, HD // 2, 1) * sine).astype(BF16)

    with jax.named_scope("rope"):
        for head in range(QPK):
            qs[head] = rope(acc[:, head * HD:(head + 1) * HD])
        knew[...] = rope(acc[:, QW:QW + HD])
        vnew[...] = acc[:, QW + HD:].astype(BF16)

    scale = (HD ** -0.5) * LOG2E
    contract = (((1,), (1,)), ((), ()))

    def score(head, keys):
        return lax.dot_general(qs[head], keys, contract, preferred_element_type=F32)

    def merge(head, scores, values):
        width = scores.shape[1]
        m_old = mrow[head]
        m_new = jnp.maximum(m_old, jnp.max(scores, axis=1, keepdims=True))
        fix = jnp.exp2((m_old - m_new) * scale)
        e = jnp.exp2((scores - m_new[:, :1]) * scale)
        l_new = lrow[head] * fix
        for j in range(width // HD):
            l_new = l_new + e[:, j * HD:(j + 1) * HD]
        oacc[head] = oacc[head] * fix + jnp.dot(
            e.astype(BF16), values, preferred_element_type=F32
        )
        mrow[head] = m_new
        lrow[head] = l_new

    kt = cfg["kt"]
    steps = L // kt
    per = CORES * LS // kt
    stages = [(0, stage_z, (1, True)), (1, inject, (4,)), (1, stage_home_y, ())]
    for t in range(1, N - 1):
        stages.append((steps - 1, stage_xg, (t, False)))
        stages.append((steps + 1, stage_d, (t, False)))
        stages.append((1 if t > 1 else steps - 1, stage_xg, (t, True)))
        stages.append((steps + 2 + (N - 2 - t) * 3, stage_d, (t, True)))
    stages.append((steps - 1, stage_z, (N - 1, True)))
    stages.append((steps + 3, stage_xg, (N - 1, True)))
    stages.append((steps + 3 * N, stage_d, (N - 1, True)))
    places = {}
    for key, stage, args in stages:
        places.setdefault(key, []).append(functools.partial(stage, *args))

    def pump(key):
        with jax.named_scope(f"pump_{key}"):
            for stage in places.pop(key, []):
                stage()

    def fits(place):
        return (place >= 0) & (place < N)

    def held(place):
        return jnp.clip(place, 0, N - 1)

    def attended(t, sign, head):
        view = abuf.at[held(z - sign * t), :, pl.ds(head * HD, HD)]
        return copies.make(("a", sign, t, head), view, view, dev(head=held(z + sign)))

    def receive(t, sign, head, cond):
        h = z - sign * t
        cond = cond & fits(h)

        @pl.when(cond)
        def _():
            view = abuf.at[held(h), :, pl.ds(head * HD, HD)]
            arrived(("a", sign, t - 1, head), view)
        if t < N - 1:
            begin(cond & fits(z + sign), functools.partial(attended, t, sign, head))

    def receive_all(t, sign, cond):
        for head in range(QPK):
            receive(t, sign, head, cond)

    def attend(i, last):
        chip = lax.rem(x + i // per, X)
        rows = pl.ds(pl.multiple_of(chip * (CORES * LS) + i % per * kt, kt), kt)
        keys, values = kvbuf[0, rows, :], kvbuf[1, rows, :]
        ahead = score(0, keys)
        for head in range(QPK):
            scores = ahead
            if head + 1 < QPK:
                ahead = score(head + 1, keys)
            merge(head, scores, values)
            if last:
                whole = jnp.sum(lrow[head], axis=1, keepdims=True)
                share = jnp.where(live, jnp.broadcast_to(1.0 / whole, (T, HD)), 0.0)
                blended = oacc[head] * share
                abuf[z, :, head * HD:(head + 1) * HD] = blended.astype(BF16)
                for sign in (1, -1):
                    begin(fits(z + sign), functools.partial(attended, 0, sign, head))

    length = length_ref[0]
    token = lax.broadcasted_iota(jnp.int32, (T, T), 0)
    place = lax.broadcasted_iota(jnp.int32, (T, T), 1)
    allowed = (place <= token) & (place < length)
    live = lax.broadcasted_iota(jnp.int32, (T, HD), 0) < length
    with jax.named_scope("self"):
        keys, values = knew[...], vnew[...]
        for head in range(QPK):
            scores = score(head, keys)
            merge(head, jnp.where(allowed, scores, FLOOR_SCORE), values)

    with jax.named_scope("kv_own"):
        cached.finish_own()
    for i in range(steps):
        if i == per:
            with jax.named_scope("kv_rest"):
                cached.finish_rest()
        with jax.named_scope(f"attend_{i}"):
            attend(i, i == steps - 1)
        pump(i)

    tn = cfg["tn"]

    def product(t, ends):
        for h, valid in sources(t):
            if t:
                valid = valid & (outer(h) == ends)

            @pl.when(valid)
            def _():
                def tile(i, _):
                    cols = pl.ds(pl.multiple_of(i * tn, tn), tn)
                    w = wobuf[h, i * tn // DS, :, pl.ds(pl.multiple_of(i * tn % DS, tn), tn)]
                    part = jnp.dot(abuf[h], w, preferred_element_type=F32)
                    total_out[:, cols] = part if t == 0 else total_out[:, cols] + part
                    return 0

                lax.fori_loop(0, W // tn, tile, 0)

    with jax.named_scope("relay_inner"):
        for t in range(1, N):
            for sign in (1, -1):
                inner = jnp.logical_not(outer(z - sign * t)) & jnp.logical_not(outer(z))
                receive_all(t, sign, inner)
    with jax.named_scope("product_0"):
        home_finish()
        product(0, False)

    def inner_product(t):
        with jax.named_scope(f"finish_{t}"):
            stage_f(t)
            for sign in (1, -1):
                receive_all(t, sign, jnp.logical_not(outer(z - sign * t)) & outer(z))
        with jax.named_scope(f"product_{t}"):
            product(t, False)

    for key in sorted(places)[:-1]:
        pump(key)
    for t in range(1, N - 1):
        inner_product(t)
    pump(steps + 3 * N)
    inner_product(N - 1)
    events = []
    for t in range(1, N):
        for head in range(QPK):
            for sign in (1, -1):
                events.append((3.5 * t + 1.4 * head, t, sign, head))
    events.sort(key=lambda event: event[0])
    with jax.named_scope("relay_outer"):
        for _, t, sign, head in events:
            receive(t, sign, head, outer(z - sign * t))
    for t in range(1, N):
        with jax.named_scope(f"product_end_{t}"):
            product(t, True)
    with jax.named_scope("final_cast"):
        out[...] = total_out[...].astype(BF16)

    for copy in sent:
        copy.wait_send()
    for t in range(N - 1):
        @pl.when((z - t >= 0) & (z + 1 < N))
        def _():
            hidden_up(t).wait_send()

        @pl.when((z + t < N) & (z > 0))
        def _():
            hidden_down(t).wait_send()
    for step in range(1, N):
        stats_copy(step).wait_send()
    for cond, make in later:
        @pl.when(cond)
        def _():
            make().wait_send()


def per_device(cfg, *args):
    hidden, lengths, pk, pv, wq, wk, wv, wo = args
    T, W = hidden.shape
    HD = pk.shape[1]
    QW = wq.shape[1]
    G, S, N = cfg["G"], cfg["S"], cfg["N"]
    D = W * N
    X = S // CORES
    B = S // N
    L = pk.shape[0] * S
    DS = D // S
    Q = max(1, 4 // max(1, X - 1))
    QK = max(1, 2 // max(1, X - 1))
    cfg = dict(
        cfg, T=T, D=D, HD=HD, QPK=QW // HD, L=L, Q=Q, QK=QK,
        tk=min(2048, W, DS), kt=min(2048, CORES * L // S), tn=min(512, W, DS),
    )
    QPK = QW // HD
    cosine, sine = tables(L, T, HD)
    copies = (
        2 + (X - 1) * Q * 2 * G + (X - 1) * QK * 2 + 2 * N
        + N * B * (1 + 3 * X * G) + 3 * X + 1 + B * (2 + 2 * G) + 2 * N * QPK + 2 * N
    )
    anywhere = pl.BlockSpec(memory_space=pl.ANY)
    vmem = pl.BlockSpec(memory_space=pltpu.VMEM)
    return pl.pallas_call(
        functools.partial(kernel, cfg),
        out_shape=jax.ShapeDtypeStruct((T, W), BF16),
        in_specs=[pl.BlockSpec(memory_space=pltpu.SMEM), vmem, vmem] + [anywhere] * 7,
        out_specs=vmem,
        scratch_shapes=[
            pltpu.VMEM((N, T, W), BF16),
            pltpu.VMEM((S, DS, QW + 2 * HD), BF16),
            pltpu.VMEM((2, L, HD), BF16),
            pltpu.VMEM((N, B, QW, DS), BF16),
            pltpu.VMEM((max(1, X - 1), QW // (G * X), DS), BF16),
            pltpu.VMEM((T, QW + 2 * HD), F32),
            pltpu.VMEM((QPK, T, HD), BF16),
            pltpu.VMEM((T, HD), BF16),
            pltpu.VMEM((T, HD), BF16),
            pltpu.VMEM((QPK, T, HD), F32),
            pltpu.VMEM((QPK, T, HD), F32),
            pltpu.VMEM((QPK, T, HD), F32),
            pltpu.VMEM((N, T, QW), BF16),
            pltpu.VMEM((T, W), F32),
            pltpu.VMEM((N, 8, T), F32),
            pltpu.VMEM((T, 128), F32),
            pltpu.SemaphoreType.DMA((copies,)),
            pltpu.SemaphoreType.DMA((copies,)),
            pltpu.SemaphoreType.DMA((7,)),
        ],
        compiler_params=pltpu.CompilerParams(
            collective_id=0, has_side_effects=True, vmem_limit_bytes=64_000_000
        ),
    )(lengths, jnp.asarray(cosine), jnp.asarray(sine), hidden, pk, pv, wq, wk, wv, wo)


def solution(mesh):
    cfg = dict(G=mesh.shape["groups"], S=mesh.shape["sample"], N=mesh.shape["head"])
    rows = P(("groups", "sample"), "head")
    placed = (
        rows, P(("groups", "sample")), rows, rows,
        P("sample", "head"), P("sample", "head"), P("sample", "head"), P("head", "sample"),
    )
    return jax.shard_map(
        functools.partial(per_device, cfg),
        mesh=mesh,
        in_specs=placed,
        out_specs=rows,
        check_vma=False,
    )
```

```python
import functools

import jax
import jax.numpy as jnp
import numpy as np
from jax import lax
from jax.experimental import pallas as pl
from jax.experimental.pallas import tpu as pltpu
from jax.sharding import PartitionSpec as P

EPSILON = 1e-06
THETA_BASE = 1000000.0
FLOOR_SCORE = -1e30
LOG2E = 1.4426950408889634
MESH = pl.DeviceIdType.MESH
F32 = jnp.float32
BF16 = jnp.bfloat16
CORES = 2


def tables(first, count, width):
    half = width // 2
    power = -(np.arange(half, dtype=np.float32) * np.float32(2.0)) / np.float32(width)
    frequency = np.power(np.float32(THETA_BASE), power, dtype=np.float32)
    places = (first + np.arange(count)).astype(np.float32)
    angles = (places[:, None] * frequency[None, :]).astype(np.float64)
    cosine = np.cos(angles).astype(np.float32)
    sine = np.sin(angles).astype(np.float32)
    return (
        np.concatenate([cosine, cosine], axis=1),
        np.concatenate([-sine, sine], axis=1),
    )


class Copies:
    def __init__(self, send, recv):
        self.send, self.recv = send, recv
        self.bases, self.size = {}, 0

    def base(self, key, count=1):
        if key not in self.bases:
            self.bases[key] = self.size
            self.size += count
        return self.bases[key]

    def put(self, src, dst, device, sent, landed):
        return pltpu.make_async_remote_copy(
            src_ref=src,
            dst_ref=dst,
            send_sem=self.send.at[sent],
            recv_sem=self.recv.at[landed],
            device_id=device,
            device_id_type=MESH,
        )

    def make(self, key, src, dst, device):
        number = self.base(key)
        return self.put(src, dst, device, number, number)


def kernel(
    cfg,
    length_ref, cos_ref, sin_ref, hid, pk, pv, wq, wk, wv, wo,
    out,
    hbuf, wall, kvbuf, wobuf, relay, acc, qs, knew, vnew, mrow, lrow, oacc, abuf, total_out,
    stats, rows,
    send_sems, recv_sems, load_sems,
):
    G, S, N, T, D, HD, QPK = cfg["G"], cfg["S"], cfg["N"], cfg["T"], cfg["D"], cfg["HD"], cfg["QPK"]
    QW = QPK * HD
    W, DS, L = D // N, D // S, cfg["L"]
    LS = L // S
    X = S // CORES
    B = S // N
    PR = QW // (G * X)
    g = lax.axis_index("groups")
    s = lax.axis_index("sample")
    z = lax.axis_index("head")
    x, c = s // CORES, s % CORES
    copies = Copies(send_sems, recv_sems)
    sent = []
    later = []

    def dev(group=None, sample=None, head=None):
        return (
            g if group is None else group,
            s if sample is None else sample,
            z if head is None else head,
        )

    partner = x * CORES + (CORES - 1 - c)

    def xpeer(step):
        return lax.rem(x + step + X, X) * CORES + c

    loads = [
        (hid, hbuf.at[z]),
        (wq, wall.at[s, :, pl.ds(0, QW)]),
        (wk, wall.at[s, :, pl.ds(QW, HD)]),
        (wv, wall.at[s, :, pl.ds(QW + HD, HD)]),
        (pk, kvbuf.at[0, pl.ds(pl.multiple_of(s * LS, LS), LS)]),
        (pv, kvbuf.at[1, pl.ds(pl.multiple_of(s * LS, LS), LS)]),
    ]
    loads = [
        pltpu.make_async_copy(a, b, load_sems.at[i]) for i, (a, b) in enumerate(loads)
    ]
    for load in loads:
        load.start()

    barrier = pltpu.get_barrier_semaphore()
    for dz in range(N):
        for ds in range(S):
            if dz or ds:
                there = dev(sample=lax.rem(s + ds, S), head=lax.rem(z + dz, N))
                pl.semaphore_signal(barrier, inc=1, device_id=there, device_id_type=MESH)
    for dg in range(1, G):
        there = dev(group=lax.rem(g + dg, G))
        pl.semaphore_signal(barrier, inc=1, device_id=there, device_id_type=MESH)
    with jax.named_scope("barrier"):
        pl.semaphore_wait(barrier, N * S - 1 + G - 1)

    def hidden_up(t):
        block = jnp.maximum(z - t, 0)
        view = hbuf.at[block]
        return copies.make(("hu", t), view, view, dev(head=jnp.minimum(z + 1, N - 1)))

    def hidden_down(t):
        block = jnp.minimum(z + t, N - 1)
        view = hbuf.at[block]
        return copies.make(("hd", t), view, view, dev(head=jnp.maximum(z - 1, 0)))

    def hidden_send(t):
        @pl.when((z - t >= 0) & (z + 1 < N))
        def _():
            hidden_up(t).start()

        @pl.when((z + t < N) & (z > 0))
        def _():
            hidden_down(t).start()

    def arrived(key, view):
        copies.make(key, view, view, dev(sample=partner)).wait_recv()

    def hidden_pump(t):
        @pl.when(z - t >= 0)
        def _():
            arrived(("hu", t - 1), hbuf.at[jnp.maximum(z - t, 0)])

            if t < N - 1:
                @pl.when(z + 1 < N)
                def _():
                    hidden_up(t).start()

        @pl.when(z + t < N)
        def _():
            arrived(("hd", t - 1), hbuf.at[jnp.minimum(z + t, N - 1)])

            if t < N - 1:
                @pl.when(z > 0)
                def _():
                    hidden_down(t).start()

    class Flow:
        def __init__(self, name, view, rows, parts, subs):
            self.name, self.view, self.rows, self.parts, self.subs = name, view, rows, parts, subs

        def piece(self, owner, part, q):
            size = self.rows // (self.parts * self.subs)
            return self.view(owner, pl.multiple_of((part * self.subs + q) * size, size), size)

        def owner(self, dx, core=None):
            return lax.rem(x - dx + X, X) * CORES + (c if core is None else core)

        def part(self, dg):
            return lax.rem(g - dg + G, G) if self.parts > 1 else 0

        def start(self):
            for q in range(self.subs):
                for dx in range(1, X):
                    piece = self.piece(s, self.part(0), q)
                    copy = copies.make((self.name, "x", dx, q), piece, piece, dev(sample=xpeer(dx)))
                    copy.start()
                    sent.append(copy)
            whole = self.view(s, 0, self.rows)
            copy = copies.make((self.name, "own"), whole, whole, dev(sample=partner))
            copy.start()
            sent.append(copy)

        def to_core(self, dx, dg, q):
            piece = self.piece(self.owner(dx), self.part(dg), q)
            copy = copies.make((self.name, "c", dx, dg, q), piece, piece, dev(sample=partner))
            copy.start()
            sent.append(copy)

        def pump_x(self, q):
            for dx in range(1, X):
                piece = self.piece(self.owner(dx), self.part(0), q)
                arrived((self.name, "x", dx, q), piece)
                for dg in range(1, self.parts):
                    copy = copies.make(
                        (self.name, "g", dx, dg, q), piece, piece, dev(group=lax.rem(g + dg, G))
                    )
                    copy.start()
                    sent.append(copy)
                self.to_core(dx, 0, q)

        def pump_g(self, q):
            for dx in range(1, X):
                for dg in range(1, self.parts):
                    arrived((self.name, "g", dx, dg, q), self.piece(self.owner(dx), self.part(dg), q))
                    self.to_core(dx, dg, q)

        def finish_own(self):
            arrived((self.name, "own"), self.view(partner, 0, self.rows))

        def finish_rest(self):
            for q in range(self.subs):
                for dx in range(1, X):
                    for dg in range(self.parts):
                        piece = self.piece(self.owner(dx, CORES - 1 - c), self.part(dg), q)
                        arrived((self.name, "c", dx, dg, q), piece)

    Q, QK = cfg["Q"], cfg["QK"]
    weights = Flow("w", lambda o, a, b: wall.at[o, pl.ds(a, b)], DS, G, Q)
    cached = Flow(
        "kv", lambda o, a, b: kvbuf.at[:, pl.ds(pl.multiple_of(o * LS + a, b), b)], LS, 1, QK
    )

    def outer(place):
        return (place == 0) | (place == N - 1)

    def piece_rows(gi, xi):
        return pl.ds(pl.multiple_of((gi * X + xi) * PR, PR), PR)

    def piece(h, b, gi, xi):
        return wobuf.at[h, b, piece_rows(gi, xi)]

    def mine(b):
        return lax.rem(z * B + b, CORES) == c

    def wo_number(kind, h):
        return copies.base(kind, N) + h

    def cut(view, half):
        return view if half is None else view.at[pl.ds(half * (PR // 2), PR // 2)]

    def corner(t):
        return {"wg": 0, "wx": 1}

    def wo_copy(kind, h, b, gi, xi, device, half=None):
        view = cut(piece(h, b, gi, xi), half)
        number = wo_number(kind, h)
        return copies.put(view, view, device, number, number)

    def begin(cond, make):
        later.append((cond, make))

        @pl.when(cond)
        def _():
            make().start()

    def gsrc(dg):
        return lax.rem(g - dg + G, G)

    def xsrc(dx):
        return lax.rem(x - dx + X, X)

    def to_x(h, b, dx, dg, half=None):
        return functools.partial(
            wo_copy, ("wx", b, dx, dg), h, b, gsrc(dg), x, dev(sample=xpeer(dx)), half
        )

    def to_g(h, b, dx, dg, half=None):
        there = dev(group=lax.rem(g + dg, G))
        return functools.partial(
            wo_copy, ("wg", b, dx, dg), h, b, g, xsrc(dx), there, half
        )

    def to_c(h, b, dx, dg):
        return functools.partial(
            wo_copy, ("wc", b, dx, dg), h, b, gsrc(dg), xsrc(dx), dev(sample=partner)
        )

    def landed(kind, h, b, gi, xi, half=None):
        view = cut(piece(h, b, gi, xi), half)
        number = wo_number(kind, h)
        copies.put(view, view, dev(sample=partner), number, number).wait_recv()

    def sources(t):
        if t == 0:
            return [(z, z >= 0)]
        return [(jnp.maximum(z - t, 0), z - t >= 0), (jnp.minimum(z + t, N - 1), z + t < N)]

    HR = QW // G
    home = s // B == z
    home_block = wobuf.at[z, lax.rem(s, B)]
    own_wo = pltpu.make_async_copy(wo, home_block, load_sems.at[len(loads)])

    def home_rows(gi):
        return pl.ds(pl.multiple_of(gi * HR, HR), HR)

    def at_home(b):
        return x == (z * B + b) // CORES

    def home_x(dx):
        landing = copies.base("oh", B) + lax.rem(s, B)
        return copies.put(
            wo.at[home_rows(g)], home_block.at[home_rows(g)], dev(sample=xpeer(dx)),
            copies.base(("ohs", dx)), landing,
        )

    def home_own():
        landing = copies.base("oo", B) + lax.rem(s, B)
        return copies.put(wo, home_block, dev(sample=partner), copies.base("oos"), landing)

    def home_copy(key, b, gi, device):
        view = wobuf.at[z, b, home_rows(gi)]
        return copies.make(key, view, view, device)

    def home_landed(number, view):
        copies.put(view, view, dev(sample=partner), number, number).wait_recv()

    def stage_home_x():
        for b in range(B):
            cond = mine(b) & jnp.logical_not(at_home(b))

            @pl.when(cond)
            def _():
                home_landed(copies.base("oh", B) + b, wobuf.at[z, b, home_rows(g)])
            for dg in range(1, G):
                begin(cond, functools.partial(
                    home_copy, ("og", b, dg), b, g, dev(group=lax.rem(g + dg, G))
                ))
            begin(cond, functools.partial(home_copy, ("oc", b, 0), b, g, dev(sample=partner)))

    def stage_home_y():
        for b in range(B):
            cond = mine(b) & jnp.logical_not(at_home(b))
            for dg in range(1, G):
                @pl.when(cond)
                def _():
                    number = copies.base(("og", b, dg))
                    home_landed(number, wobuf.at[z, b, home_rows(gsrc(dg))])
                begin(cond, functools.partial(
                    home_copy, ("oc", b, dg), b, gsrc(dg), dev(sample=partner)
                ))

    def home_finish():
        @pl.when(home)
        def _():
            own_wo.wait()
        for b in range(B):
            @pl.when(jnp.logical_not(mine(b)) & at_home(b))
            def _():
                home_landed(copies.base("oo", B) + b, wobuf.at[z, b])

            @pl.when(jnp.logical_not(mine(b)) & jnp.logical_not(at_home(b)))
            def _():
                for dg in range(G):
                    number = copies.base(("oc", b, dg))
                    home_landed(number, wobuf.at[z, b, home_rows(gsrc(dg))])

    def stage_z(t, outer_plane):
        for h, valid in sources(t):
            for b in range(B):
                cond = valid & mine(b) & (outer(z) == outer_plane)

                @pl.when(cond)
                def _():
                    landed(("wz", b), h, b, g, x)
                for dx in range(1, X):
                    begin(cond, to_x(h, b, dx, 0))
                for dg in range(1, G):
                    begin(cond, to_g(h, b, 0, dg))
                begin(cond, to_c(h, b, 0, 0))

    def stage_xg(t, outer_plane):
        for h, valid in sources(t):
            for b in range(B):
                cond = valid & mine(b) & (outer(z) == outer_plane)
                for dx in range(1, X):
                    @pl.when(cond)
                    def _():
                        landed(("wx", b, dx, 0), h, b, g, xsrc(dx))
                    if "wg" in corner(t):
                        for dg in range(1, G):
                            begin(cond, to_g(h, b, dx, dg, corner(t)["wg"]))
                    begin(cond, to_c(h, b, dx, 0))
                for dg in range(1, G):
                    @pl.when(cond)
                    def _():
                        landed(("wg", b, 0, dg), h, b, gsrc(dg), x)
                    if "wx" in corner(t):
                        for dx in range(1, X):
                            begin(cond, to_x(h, b, dx, dg, corner(t)["wx"]))
                    begin(cond, to_c(h, b, 0, dg))

    def stage_d(t, outer_plane):
        for h, valid in sources(t):
            for b in range(B):
                cond = valid & mine(b) & (outer(z) == outer_plane)
                for dx in range(1, X):
                    for dg in range(1, G):
                        @pl.when(cond)
                        def _():
                            for kind, half in corner(t).items():
                                landed((kind, b, dx, dg), h, b, gsrc(dg), xsrc(dx), half)
                        begin(cond, to_c(h, b, dx, dg))

    def stage_f(t):
        for h, valid in sources(t):
            for b in range(B):
                @pl.when(valid & jnp.logical_not(mine(b)))
                def _():
                    for dx in range(X):
                        for dg in range(G):
                            landed(("wc", b, dx, dg), h, b, gsrc(dg), xsrc(dx))

    def cross(dx):
        to = lax.rem(x + dx, X)
        number = copies.base(("wr", dx))
        return copies.put(
            wo.at[piece_rows(g, to)], relay.at[dx - 1], dev(sample=xpeer(dx)), number, number
        )

    def along(dx):
        o = xsrc(dx) * CORES + c
        p, b = o // B, lax.rem(o, B)
        src = wo.at[piece_rows(g, x)] if dx == 0 else relay.at[dx - 1]
        landing = copies.base(("wz", 0), N * B) + b * N + z
        return copies.put(
            src, piece(z, b, g, x), dev(head=p), copies.base(("wzs", dx)), landing
        )

    for b in range(1, B):
        copies.bases[("wz", b)] = copies.base(("wz", 0), N * B) + b * N
    copies.base(("wz", 0), N * B)

    def inject(stage):
        end = (z == 0) | (z == N - 1)
        for dx in range(X):
            p = (xsrc(dx) * CORES + c) // B
            far = jnp.abs(p - z)
            early = jnp.where(far == 1, 1, jnp.where(far < N - 1, 2, 4))
            when = jnp.where(end, early, 2)
            if dx:
                when = jnp.maximum(when, 2)
            cond = (far > 0) & (when == stage)
            if dx:
                @pl.when(cond)
                def _():
                    number = copies.base(("wr", dx))
                    view = relay.at[dx - 1]
                    copies.put(view, view, dev(sample=partner), number, number).wait_recv()
            begin(cond, functools.partial(along, dx))

    loads[0].wait()
    hidden_send(0)
    for i in (1, 2, 3):
        loads[i].wait()
    weights.start()
    for dx in range(1, X):
        begin(home, functools.partial(home_x, dx))
    begin(home, home_own)

    @pl.when(home)
    def _():
        own_wo.start()
    for dx in range(1, X):
        begin(jnp.logical_not(home), functools.partial(cross, dx))
    for i in (4, 5):
        loads[i].wait()
    cached.start()

    mrow[...] = jnp.full_like(mrow, FLOOR_SCORE)
    lrow[...] = jnp.zeros_like(lrow)
    oacc[...] = jnp.zeros_like(oacc)

    tk = cfg["tk"]

    def stats_copy(step):
        view = stats.at[z]
        landing = copies.base("st", N) + z
        there = dev(head=lax.rem(z + step, N))
        return copies.put(view, view, there, copies.base(("sts", step)), landing)

    def stats_send():
        part = jnp.zeros((T, 128), F32)
        for j in range(W // 128):
            h = hbuf[z, :, j * 128:(j + 1) * 128].astype(F32)
            part = part + h * h
        part = jnp.sum(jnp.transpose(part), axis=0, keepdims=True)
        stats[z] = jnp.broadcast_to(part, (8, T))
        for step in range(1, N):
            stats_copy(step).start()

    def stats_factor():
        for step in range(1, N):
            h = lax.rem(z + step, N)
            view = stats.at[h]
            number = copies.base("st", N) + h
            copies.put(view, view, dev(sample=partner), number, number).wait_recv()
        total = stats[0]
        for h in range(1, N):
            total = total + stats[h]
        scale = lax.rsqrt(total * (1.0 / D) + EPSILON)
        rows[...] = jnp.transpose(jnp.broadcast_to(scale[:1], (128, T)))

    def project(t):
        for h, valid in sources(t):
            @pl.when(valid)
            def _():
                factor = rows[:, :1]

                def part(i, _):
                    first = h * W + i * tk
                    n = hbuf[h, :, pl.ds(pl.multiple_of(i * tk, tk), tk)].astype(F32)
                    n = (n * factor).astype(BF16)
                    w = wall[first // DS, pl.ds(pl.multiple_of(first % DS, tk), tk), :]
                    dot = jnp.dot(n, w, preferred_element_type=F32)
                    acc[...] = dot + (acc[...] if t else jnp.where(i > 0, acc[...], 0.0))
                    return 0

                lax.fori_loop(0, W // tk, part, 0)

    def project_early():
        weights.finish_own()
        weights.finish_rest()
        stats_factor()
        for t in range(N - 1):
            project(t)

    jobs = []
    for q in range(Q):
        jobs.append(((q + 1) * 8.4 * 4 / Q, functools.partial(weights.pump_x, q)))
        jobs.append(((q + 2) * 8.4 * 4 / Q + 0.5, functools.partial(weights.pump_g, q)))
    for t in range(1, N):
        jobs.append((t * 22.0, functools.partial(hidden_pump, t)))
    for q in range(QK - 1):
        jobs.append((51 + (q + 1) * 22.0 / QK, functools.partial(cached.pump_x, q)))
    jobs.append((24, functools.partial(inject, 1)))
    jobs.append((47, stage_home_x))
    jobs.append((52, functools.partial(inject, 2)))
    for t in range(2, N - 1):
        jobs.append((65 - t / N, functools.partial(stage_z, t, True)))
    for t in range(1, N - 1):
        jobs.append((63 + t / N, functools.partial(stage_z, t, False)))
    jobs.append((1, stats_send))
    jobs.append((max(60, (N - 2) * 22 + 1), project_early))
    jobs.append((65.2, functools.partial(cached.pump_x, QK - 1)))
    jobs.sort(key=lambda job: job[0])
    for when, job in jobs:
        with jax.named_scope(f"job_{when}"):
            job()
    with jax.named_scope("project"):
        project(N - 1)
    cosine, sine = cos_ref[...], sin_ref[...]

    def rope(v):
        return (v * cosine + pltpu.roll(v, HD // 2, 1) * sine).astype(BF16)

    with jax.named_scope("rope"):
        for head in range(QPK):
            qs[head] = rope(acc[:, head * HD:(head + 1) * HD])
        knew[...] = rope(acc[:, QW:QW + HD])
        vnew[...] = acc[:, QW + HD:].astype(BF16)

    scale = (HD ** -0.5) * LOG2E
    contract = (((1,), (1,)), ((), ()))

    def score(head, keys):
        return lax.dot_general(qs[head], keys, contract, preferred_element_type=F32)

    def merge(head, scores, values):
        width = scores.shape[1]
        m_old = mrow[head]
        m_new = jnp.maximum(m_old, jnp.max(scores, axis=1, keepdims=True))
        fix = jnp.exp2((m_old - m_new) * scale)
        e = jnp.exp2((scores - m_new[:, :1]) * scale)
        l_new = lrow[head] * fix
        for j in range(width // HD):
            l_new = l_new + e[:, j * HD:(j + 1) * HD]
        oacc[head] = oacc[head] * fix + jnp.dot(
            e.astype(BF16), values, preferred_element_type=F32
        )
        mrow[head] = m_new
        lrow[head] = l_new

    kt = cfg["kt"]
    steps = L // kt
    per = CORES * LS // kt
    stages = [(0, stage_z, (1, True)), (0, inject, (4,)), (1, stage_home_y, ())]
    for t in range(1, N - 1):
        stages.append((steps - 1, stage_xg, (t, False)))
        stages.append((steps + 1, stage_d, (t, False)))
        stages.append((1 if t > 1 else min(2, steps - 1), stage_xg, (t, True)))
        stages.append((steps + 2 + (N - 2 - t) * 3, stage_d, (t, True)))
    stages.append((steps - 1, stage_z, (N - 1, True)))
    stages.append((steps + 3, stage_xg, (N - 1, True)))
    stages.append((steps + 3 * N, stage_d, (N - 1, True)))
    places = {}
    for key, stage, args in stages:
        places.setdefault(key, []).append(functools.partial(stage, *args))

    def pump(key):
        with jax.named_scope(f"pump_{key}"):
            for stage in places.pop(key, []):
                stage()

    def fits(place):
        return (place >= 0) & (place < N)

    def held(place):
        return jnp.clip(place, 0, N - 1)

    def attended(t, sign, head):
        view = abuf.at[held(z - sign * t), :, pl.ds(head * HD, HD)]
        return copies.make(("a", sign, t, head), view, view, dev(head=held(z + sign)))

    def receive(t, sign, head, cond):
        h = z - sign * t
        cond = cond & fits(h)

        @pl.when(cond)
        def _():
            view = abuf.at[held(h), :, pl.ds(head * HD, HD)]
            arrived(("a", sign, t - 1, head), view)
        if t < N - 1:
            begin(cond & fits(z + sign), functools.partial(attended, t, sign, head))

    def receive_all(t, sign, cond):
        for head in range(QPK):
            receive(t, sign, head, cond)

    def attend(i, last):
        chip = lax.rem(x + i // per, X)
        rows = pl.ds(pl.multiple_of(chip * (CORES * LS) + i % per * kt, kt), kt)
        keys, values = kvbuf[0, rows, :], kvbuf[1, rows, :]
        ahead = score(0, keys)
        for head in range(QPK):
            scores = ahead
            if head + 1 < QPK:
                ahead = score(head + 1, keys)
            merge(head, scores, values)
            if last:
                whole = jnp.sum(lrow[head], axis=1, keepdims=True)
                share = jnp.where(live, jnp.broadcast_to(1.0 / whole, (T, HD)), 0.0)
                blended = oacc[head] * share
                abuf[z, :, head * HD:(head + 1) * HD] = blended.astype(BF16)
                for sign in (1, -1):
                    begin(fits(z + sign), functools.partial(attended, 0, sign, head))

    length = length_ref[0]
    token = lax.broadcasted_iota(jnp.int32, (T, T), 0)
    place = lax.broadcasted_iota(jnp.int32, (T, T), 1)
    allowed = (place <= token) & (place < length)
    live = lax.broadcasted_iota(jnp.int32, (T, HD), 0) < length
    with jax.named_scope("self"):
        keys, values = knew[...], vnew[...]
        for head in range(QPK):
            scores = score(head, keys)
            merge(head, jnp.where(allowed, scores, FLOOR_SCORE), values)

    with jax.named_scope("kv_own"):
        cached.finish_own()
    for i in range(steps):
        if i == per:
            with jax.named_scope("kv_rest"):
                cached.finish_rest()
        with jax.named_scope(f"attend_{i}"):
            attend(i, i == steps - 1)
        pump(i)

    tn = cfg["tn"]

    def product(t, ends):
        for h, valid in sources(t):
            if t:
                valid = valid & (outer(h) == ends)

            @pl.when(valid)
            def _():
                def tile(i, _):
                    cols = pl.ds(pl.multiple_of(i * tn, tn), tn)
                    w = wobuf[h, i * tn // DS, :, pl.ds(pl.multiple_of(i * tn % DS, tn), tn)]
                    part = jnp.dot(abuf[h], w, preferred_element_type=F32)
                    total_out[:, cols] = part if t == 0 else total_out[:, cols] + part
                    return 0

                lax.fori_loop(0, W // tn, tile, 0)

    with jax.named_scope("relay_inner"):
        for t in range(1, N):
            for sign in (1, -1):
                inner = jnp.logical_not(outer(z - sign * t)) & jnp.logical_not(outer(z))
                receive_all(t, sign, inner)
    events = []
    for t in range(1, N):
        for head in range(QPK):
            for sign in (1, -1):
                events.append((3.5 * t + 1.4 * head, t, sign, head))
    events.sort(key=lambda event: event[0])

    def relay_outer(outer_plane):
        for _, t, sign, head in events:
            receive(t, sign, head, outer(z - sign * t) & (outer(z) == outer_plane))

    with jax.named_scope("product_0"):
        home_finish()
        product(0, False)
    with jax.named_scope("relay_mid"):
        relay_outer(False)

    def inner_product(t):
        with jax.named_scope(f"finish_{t}"):
            stage_f(t)
            for sign in (1, -1):
                receive_all(t, sign, jnp.logical_not(outer(z - sign * t)) & outer(z))
        with jax.named_scope(f"product_{t}"):
            product(t, False)

    for key in sorted(places)[:-1]:
        pump(key)
    for t in range(1, N - 1):
        inner_product(t)
    pump(steps + 3 * N)
    inner_product(N - 1)
    with jax.named_scope("relay_outer"):
        relay_outer(True)
    for t in range(1, N):
        with jax.named_scope(f"product_end_{t}"):
            product(t, True)
    with jax.named_scope("final_cast"):
        out[...] = total_out[...].astype(BF16)

    for copy in sent:
        copy.wait_send()
    for t in range(N - 1):
        @pl.when((z - t >= 0) & (z + 1 < N))
        def _():
            hidden_up(t).wait_send()

        @pl.when((z + t < N) & (z > 0))
        def _():
            hidden_down(t).wait_send()
    for step in range(1, N):
        stats_copy(step).wait_send()
    for cond, make in later:
        @pl.when(cond)
        def _():
            make().wait_send()


def per_device(cfg, *args):
    hidden, lengths, pk, pv, wq, wk, wv, wo = args
    T, W = hidden.shape
    HD = pk.shape[1]
    QW = wq.shape[1]
    G, S, N = cfg["G"], cfg["S"], cfg["N"]
    D = W * N
    X = S // CORES
    B = S // N
    L = pk.shape[0] * S
    DS = D // S
    Q = max(1, 4 // max(1, X - 1))
    QK = max(1, 2 // max(1, X - 1))
    cfg = dict(
        cfg, T=T, D=D, HD=HD, QPK=QW // HD, L=L, Q=Q, QK=QK,
        tk=min(2048, W, DS), kt=min(2048, CORES * L // S), tn=min(512, W, DS),
    )
    QPK = QW // HD
    cosine, sine = tables(L, T, HD)
    copies = (
        2 + (X - 1) * Q * 2 * G + (X - 1) * QK * 2 + 2 * N
        + N * B * (1 + 3 * X * G) + 3 * X + 1 + B * (2 + 2 * G) + 2 * N * QPK + 2 * N
    )
    anywhere = pl.BlockSpec(memory_space=pl.ANY)
    vmem = pl.BlockSpec(memory_space=pltpu.VMEM)
    return pl.pallas_call(
        functools.partial(kernel, cfg),
        out_shape=jax.ShapeDtypeStruct((T, W), BF16),
        in_specs=[pl.BlockSpec(memory_space=pltpu.SMEM), vmem, vmem] + [anywhere] * 7,
        out_specs=vmem,
        scratch_shapes=[
            pltpu.VMEM((N, T, W), BF16),
            pltpu.VMEM((S, DS, QW + 2 * HD), BF16),
            pltpu.VMEM((2, L, HD), BF16),
            pltpu.VMEM((N, B, QW, DS), BF16),
            pltpu.VMEM((max(1, X - 1), QW // (G * X), DS), BF16),
            pltpu.VMEM((T, QW + 2 * HD), F32),
            pltpu.VMEM((QPK, T, HD), BF16),
            pltpu.VMEM((T, HD), BF16),
            pltpu.VMEM((T, HD), BF16),
            pltpu.VMEM((QPK, T, HD), F32),
            pltpu.VMEM((QPK, T, HD), F32),
            pltpu.VMEM((QPK, T, HD), F32),
            pltpu.VMEM((N, T, QW), BF16),
            pltpu.VMEM((T, W), F32),
            pltpu.VMEM((N, 8, T), F32),
            pltpu.VMEM((T, 128), F32),
            pltpu.SemaphoreType.DMA((copies,)),
            pltpu.SemaphoreType.DMA((copies,)),
            pltpu.SemaphoreType.DMA((7,)),
        ],
        compiler_params=pltpu.CompilerParams(
            collective_id=0, has_side_effects=True, vmem_limit_bytes=64_000_000
        ),
    )(lengths, jnp.asarray(cosine), jnp.asarray(sine), hidden, pk, pv, wq, wk, wv, wo)


def solution(mesh):
    cfg = dict(G=mesh.shape["groups"], S=mesh.shape["sample"], N=mesh.shape["head"])
    rows = P(("groups", "sample"), "head")
    placed = (
        rows, P(("groups", "sample")), rows, rows,
        P("sample", "head"), P("sample", "head"), P("sample", "head"), P("head", "sample"),
    )
    return jax.shard_map(
        functools.partial(per_device, cfg),
        mesh=mesh,
        in_specs=placed,
        out_specs=rows,
        check_vma=False,
    )
```
